32 devices in a mesh: grp: 2 (over y), gx: 4 (over z), gy: 4 (over x, core).
Axes of the slice: x: 2, y: 2, z: 4, core: 2. Of those that a mesh axis runs over, the one named last changes fastest.
Arguments:
- samples: bfloat16 [2816, 65536], P('grp', ('gx', 'gy')), parts along dimension 0, may hold values from -400 to 400
- tile_owner: int32 [256], replicated, may hold values from 0 to 255, each once
Outputs:
- kernel_tiles: float32 [512, 4096], P(('grp', 'gx', 'gy')), parts along dimension 0
The draws below stay inside these ranges and needn't reach their ends.
There are 2 independent parts, one for each index of `grp`. The reference program is written for one: setup_inputs(seed, part) draws one part's arguments, and reference() takes and returns one part's arrays. A program takes and returns all parts, laid end to end along the dimension named above; an argument that names none is the same for every part. Nothing has to cross between parts.
Inputs may be any that keep to these rules, and one draw needn't show every extreme that they name: tile_owner holds each of 0 to 255 once; device k of the group (k = gx index * 4 + gy index) owns slots k * 16 to (k + 1) * 16 - 1; values of 253 and above mark empty slots.
All inputs are finite; a program needn't handle non-finite values.
Results may differ from the reference program's by a relative error of at most 0.0003.
Values sent between devices are 32-bit elements; how exact they have to be, the bound alone decides.
No kernel may reach another device: no remote copies, remote signals or barrier semaphores. Data moves between devices by JAX's collectives and lax.ppermute only.
A program may use at most 64 MiB of HBM per device.

```python
import math
import jax
import jax.numpy as jnp
import numpy as np
from jax import lax

FEATURES = 65536
NS = 1408
TILE = 64
NT = 22
NLOW = 253
ALLSLOTS = 256


def draw_samples(key, part):
    key_rows = jax.random.fold_in(key, 11)
    key_cols = jax.random.fold_in(key, 12)
    key_base = jax.random.fold_in(key, 13)
    row_scale = jnp.exp(jax.random.uniform(key_rows, (NS, 1), jnp.float32) * math.log(10.0))
    ramp = jnp.exp(math.log(3.0) * jnp.arange(FEATURES, dtype=jnp.float32) / FEATURES)[None, :]
    col_scale = ramp * jnp.exp(jax.random.uniform(key_cols, (1, FEATURES), jnp.float32) * math.log(3.0))
    base = jnp.clip(jax.random.normal(key_base, (NS, FEATURES), jnp.float32), -4.0, 4.0)
    return (row_scale * col_scale * base).astype(jnp.bfloat16)


def setup_inputs(seed: int = 0, part: int = 0) -> dict:
    keys = jax.random.split(jax.random.key(seed), 3)
    part_keys = jax.random.split(jax.random.fold_in(keys[2], part), 3)
    return {
        "samples": draw_samples(jax.random.fold_in(jax.random.fold_in(keys[2], part), 71), part),
        "tile_owner": jax.random.permutation(keys[1], ALLSLOTS).astype(jnp.int32),
    }


def tile_coords(order):
    firsts = np.array([k * (k + 1) // 2 for k in range(1, NT)], dtype=np.int32)
    tile_row = lax.optimization_barrier(jnp.sum((order[:, None] >= jnp.asarray(firsts)[None, :]).astype(jnp.int32), axis=1)).astype(jnp.int32)
    tile_col = order - tile_row * (tile_row + 1) // 2
    is_live = order < NLOW
    tile_row = jnp.where(is_live, tile_row, 0).astype(jnp.int32)
    tile_col = jnp.where(is_live, tile_col, 0).astype(jnp.int32)
    return (tile_row, tile_col, is_live)

def reference(samples, tile_owner):
    gram = jnp.dot(samples, samples.T, preferred_element_type=jnp.float32)
    values = samples.astype(jnp.float32)
    meansq = lax.optimization_barrier(jnp.sum(values * values, axis=1)) / FEATURES + 1e-06
    inverse = 1.0 / jnp.sqrt(meansq)
    cosine = gram * inverse[:, None] * inverse[None, :] / jnp.sqrt(jnp.float32(FEATURES))
    blocked = cosine.reshape(NT, TILE, NT, TILE).transpose(0, 2, 1, 3)
    tile_row, tile_col, is_live = tile_coords(tile_owner)
    picked = blocked[tile_row, tile_col].reshape(tile_owner.shape[0], TILE * TILE)
    return picked * is_live[:, None].astype(jnp.float32)
```

```python
import functools

import jax
import jax.numpy as jnp
from jax import lax
from jax.experimental import pallas as pl
from jax.experimental.pallas import tpu as pltpu
from jax.sharding import PartitionSpec as P


TILE = 64
HALF = TILE // 2
LANES = 2 * TILE
PITCH = HALF + 8
EPS = 1e-06
AXES = ("gx", "gy")


def row_cuts(rows):
    cuts = list(range(0, rows, 256))
    if len(cuts) > 1 and rows - cuts[-1] < 256:
        cuts.pop()
    return tuple(zip(cuts, cuts[1:] + [rows]))


def gram_kernel(cuts, spans, hbm_ref, tiles, squares, x_ref, g_ref, sems):
    copies = [
        pltpu.make_async_copy(hbm_ref.at[:, pl.ds(lo, hi - lo)], x_ref.at[:, pl.ds(lo, hi - lo)], sems.at[n])
        for n, (lo, hi) in enumerate(spans)
    ]
    for copy in copies:
        copy.start()
    left = lax.broadcasted_iota(jnp.int32, (HALF, LANES), 1) < TILE
    eye = lax.broadcasted_iota(jnp.int32, (LANES, LANES), 0) == lax.broadcasted_iota(jnp.int32, (LANES, LANES), 1)
    diagonal = []
    for n, (k0, k1) in enumerate(spans):
        copies[n].wait()
        for m, (r0, r1) in enumerate(cuts):
            for c0, c1 in cuts[: m + 1]:
                block = lax.dot_general(
                    x_ref[r0:r1, k0:k1], x_ref[c0:c1, k0:k1], (((1,), (1,)), ((), ())), preferred_element_type=jnp.float32
                )
                if n:
                    block = g_ref[r0:r1, c0:c1] + block
                g_ref[r0:r1, c0:c1] = block
                if n + 1 < len(spans):
                    continue
                for row in range(r0 // TILE, r1 // TILE):
                    for b in range(c0 // LANES, c1 // LANES):
                        col = 2 * b
                        if col > row:
                            continue
                        lanes = slice(b * LANES, (b + 1) * LANES)
                        upper = g_ref[row * TILE : row * TILE + HALF, lanes]
                        lower = g_ref[row * TILE + HALF : (row + 1) * TILE, lanes]
                        at = (row * (row + 1) // 2 + col) * HALF
                        tiles[at : at + HALF, :] = jnp.where(left, upper, pltpu.roll(lower, TILE, 1))
                        if col + 1 <= row:
                            tiles[at + HALF : at + 2 * HALF, :] = jnp.where(left, pltpu.roll(upper, TILE, 1), lower)
            if n + 1 == len(spans):
                for b in range(r0 // LANES, r1 // LANES):
                    part = g_ref[b * LANES : (b + 1) * LANES, b * LANES : (b + 1) * LANES]
                    diagonal.append(jnp.sum(jnp.where(eye, part, 0.0), axis=0, keepdims=True))
    high = cuts[-1][1] // TILE
    live = high * (high + 1) // 2 * HALF
    tiles[live:, :] = jnp.zeros((tiles.shape[0] - live, LANES), jnp.float32)
    extra = squares.shape[0]
    squares[...] = jnp.concatenate(diagonal + [jnp.zeros((extra - len(diagonal), LANES), jnp.float32)], axis=0)


def gram_tiles(samples, count, extra):
    rows, features = samples.shape
    cuts = row_cuts(rows)
    first = features // 4
    spans = ((0, first), (first, features)) if first % LANES == 0 else ((0, features),)
    vmem = pl.BlockSpec(memory_space=pltpu.VMEM)
    return pl.pallas_call(
        functools.partial(gram_kernel, cuts, spans),
        out_shape=[
            jax.ShapeDtypeStruct((count * HALF, LANES), jnp.float32),
            jax.ShapeDtypeStruct((extra, LANES), jnp.float32),
        ],
        in_specs=[pl.BlockSpec(memory_space=pltpu.HBM)],
        out_specs=[vmem] * 2,
        scratch_shapes=[
            pltpu.VMEM((rows, features), samples.dtype),
            pltpu.VMEM((rows, rows), jnp.float32),
            pltpu.SemaphoreType.DMA((len(spans),)),
        ],
        compiler_params=pltpu.CompilerParams(vmem_limit_bytes=44 * 2**20),
        cost_estimate=pl.CostEstimate(
            flops=rows * rows * features, bytes_accessed=rows * features * 2 + count * HALF * LANES * 4, transcendentals=0
        ),
        name="gram_tiles",
    )(samples)


def pick_kernel(pieces, bounds, columns, slots, owner_ref, tiles, squares, *outs):
    at_x, at_y = lax.axis_index("gx"), lax.axis_index("gy")
    for out, atoms in zip(outs, pieces):
        at = 0
        for far_x, far_y, k in atoms:
            dest = (at_x ^ far_x) * columns + (at_y ^ far_y)
            lo, hi = bounds[k]
            for i in range(lo // HALF, min(hi // HALF, slots)):
                source = pl.multiple_of(owner_ref[dest * slots + i] * HALF, HALF)
                out[at : at + HALF, :] = tiles[pl.ds(source, HALF), :]
                at += HALF
            if hi == bounds[-1][1]:
                out[at : at + squares.shape[0], :] = squares[...]
                at += squares.shape[0]


def pick_tiles(owner, tiles, squares, pieces, bounds, columns, slots):
    sizes = [sum(bounds[k][1] - bounds[k][0] for _, _, k in atoms) for atoms in pieces]
    vmem, smem = pl.BlockSpec(memory_space=pltpu.VMEM), pl.BlockSpec(memory_space=pltpu.SMEM)
    return pl.pallas_call(
        functools.partial(pick_kernel, pieces, bounds, columns, slots),
        out_shape=[jax.ShapeDtypeStruct((size, LANES), jnp.float32) for size in sizes],
        in_specs=[smem, vmem, vmem],
        out_specs=[vmem] * len(sizes),
        compiler_params=pltpu.CompilerParams(vmem_limit_bytes=2**20),
        cost_estimate=pl.CostEstimate(flops=10**6, bytes_accessed=sum(sizes) * LANES * 8, transcendentals=0),
        name="pick_tiles",
    )(owner, tiles, squares)


def finish_kernel(joined, slots, features, index_ref, *refs):
    out_ref, total, inv, rows_of, cols_of, packed = refs[-6:]
    add_kernel(joined, *refs[:-6], total)
    meansq = total[slots * HALF :, :] / features + EPS
    inv[...] = 1.0 / jnp.sqrt(meansq)
    half = lax.broadcasted_iota(jnp.int32, (1, LANES), 1) < TILE

    def pick(tile):
        line = inv[pl.ds(lax.div(tile, 2), 1), :]
        turned = pltpu.roll(line, TILE, 1)
        odd = lax.rem(tile, 2) == 1
        return jnp.where(odd, turned, line), jnp.where(odd, line, turned)

    rows_of[...] = jnp.zeros_like(rows_of)
    for i in range(slots):
        first, second = pick(index_ref[i])
        rows_of[i : i + 1, :] = first
        first, second = pick(index_ref[slots + i])
        alive = index_ref[2 * slots + i] == 1
        cols_of[i : i + 1, :] = jnp.where(half, first, second)
    down = rows_of[...].T
    left = lax.broadcasted_iota(jnp.int32, (HALF, LANES), 1) < TILE
    norm = 1.0 / features**0.5
    for i in range(slots):
        by_row = jnp.where(left, down[:HALF, i : i + 1], down[HALF:TILE, i : i + 1])
        scaled = total[i * HALF : (i + 1) * HALF, :] * by_row * (cols_of[i : i + 1, :] * norm)
        alive = index_ref[2 * slots + i] == 1
        packed[i * PITCH : i * PITCH + HALF, :] = jnp.where(alive, scaled, 0.0)
    step = min(slots, 8)
    wide = lax.broadcasted_iota(jnp.int32, (step, LANES), 1) < TILE
    for s in range(0, slots, step):
        for j in range(HALF):
            q = (2 * j) % HALF
            even = packed[pl.ds(s * PITCH + q, step, stride=PITCH), :]
            odd = packed[pl.ds(s * PITCH + q + 1, step, stride=PITCH), :]
            if 2 * j < HALF:
                line = jnp.where(wide, even, pltpu.roll(odd, TILE, 1))
            else:
                line = jnp.where(wide, pltpu.roll(even, TILE, 1), odd)
            out_ref[s : s + step, j * LANES : (j + 1) * LANES] = line


def finish(index, arrays, joined, slots, features):
    per = sum(size for _, size in joined)
    extra = per - slots * HALF
    vmem = pl.BlockSpec(memory_space=pltpu.VMEM)
    return pl.pallas_call(
        functools.partial(finish_kernel, joined, slots, features),
        out_shape=jax.ShapeDtypeStruct((slots, TILE * TILE), jnp.float32),
        in_specs=[pl.BlockSpec(memory_space=pltpu.SMEM)] + [vmem] * len(arrays),
        out_specs=vmem,
        scratch_shapes=[
            pltpu.VMEM((per, LANES), jnp.float32),
            pltpu.VMEM((extra, LANES), jnp.float32),
            pltpu.VMEM((LANES, LANES), jnp.float32),
            pltpu.VMEM((max(slots, 8), LANES), jnp.float32),
            pltpu.VMEM((slots * PITCH, LANES), jnp.float32),
        ],
        compiler_params=pltpu.CompilerParams(vmem_limit_bytes=6 * 2**20),
        cost_estimate=pl.CostEstimate(flops=per * LANES * 8, bytes_accessed=per * LANES * 32, transcendentals=0),
        name="finish_tiles",
    )(index, *arrays)


def add_kernel(joined, *refs):
    at = 0
    for parts, size in joined:
        value = refs[parts[0][0]][parts[0][1] : parts[0][1] + size, :]
        for i, lo in parts[1:]:
            value = value + refs[i][lo : lo + size, :]
        refs[-1][at : at + size, :] = value
        at += size


def add_terms(arrays, joined):
    rows = sum(size for _, size in joined)
    vmem = pl.BlockSpec(memory_space=pltpu.VMEM)
    return pl.pallas_call(
        functools.partial(add_kernel, joined),
        out_shape=jax.ShapeDtypeStruct((rows, LANES), jnp.float32),
        in_specs=[vmem] * len(arrays),
        out_specs=vmem,
        compiler_params=pltpu.CompilerParams(vmem_limit_bytes=2 * 2**20),
        cost_estimate=pl.CostEstimate(flops=rows * LANES * 3, bytes_accessed=rows * LANES * 16, transcendentals=0),
        name="add_terms",
    )(*arrays)


def index_kernel(slots, columns, firsts, owner_ref, out_ref):
    at = (lax.axis_index("gx") * columns + lax.axis_index("gy")) * slots
    for i in range(slots):
        tile = owner_ref[at + i]
        row = jnp.int32(0)
        for first in firsts[1:-1]:
            row = row + (tile >= first).astype(jnp.int32)
        alive = tile < firsts[-1]
        out_ref[i] = jnp.where(alive, row, 0)
        out_ref[slots + i] = jnp.where(alive, tile - row * (row + 1) // 2, 0)
        out_ref[2 * slots + i] = alive.astype(jnp.int32)


def tile_index(owner, slots, columns, side):
    smem = pl.BlockSpec(memory_space=pltpu.SMEM)
    firsts = tuple(k * (k + 1) // 2 for k in range(side + 1))
    return pl.pallas_call(
        functools.partial(index_kernel, slots, columns, firsts),
        out_shape=jax.ShapeDtypeStruct((3 * slots,), jnp.int32),
        in_specs=[smem],
        out_specs=smem,
        compiler_params=pltpu.CompilerParams(vmem_limit_bytes=2**20),
        cost_estimate=pl.CostEstimate(flops=10**6, bytes_accessed=2**10, transcendentals=0),
        name="tile_index",
    )(owner)


def cut(per, parts):
    total = sum(parts)
    marks = [0]
    for part in parts:
        marks.append(marks[-1] + part)
    marks = [mark * per // total // HALF * HALF for mark in marks[:-1]] + [per]
    return list(zip(marks, marks[1:]))


def halving(gx, gy, per):
    bounds = cut(per, [1])
    blocks = [(x, y, 0) for y in range(gy) for x in range(gx)]
    pieces, sends = [], []
    for axis, size in (("gy", gy), ("gx", gx)):
        for bit in (1 << b for b in range(size.bit_length() - 1)):
            far = [block for block in blocks if (block[1] if axis == "gy" else block[0]) & bit]
            blocks = [block for block in blocks if block not in far]
            pieces = pieces or [(0, [far]), (1, [blocks])]
            sends.append((axis, bit, far))
    return bounds, pieces, sends


def plan(gx, gy, per):
    if (gx, gy) != (4, 4):
        return halving(gx, gy, per)
    core, x, z, zz = ("gy", 1), ("gy", 2), ("gx", 1), ("gx", 2)
    bounds = cut(per, [1, 3])
    sent = [
        [(3, 3, 1)],
        [(3, 3, 0), (1, 3, 0), (3, 1, 0), (1, 1, 0)],
        [(2, 3, 1)],
        [(1, 3, 1), (0, 3, 1)],
        [(2, 3, 0), (2, 1, 0), (0, 3, 0), (0, 1, 0)],
        [(r, 1, 1) for r in range(4)],
    ]
    kept = [[(r, y & 2, k) for r, y, k in atoms] for atoms in sent]
    groups = [(0, sent), (2, kept)]
    first, second, *others = [(*core, atoms) for atoms in sent]
    sends = [first, second, (*x, [(3, 2, 1)]), (*z, [(3, 2, 0), (1, 2, 0), (3, 0, 0), (1, 0, 0)]), *others]
    sends += [(*x, [(r, 2, 1)]) for r in (2, 1, 0)]
    sends += [(*z, [(3, 0, 1)]), (*zz, [(2, 2, 0), (2, 0, 0)]), (*zz, [(2, 0, 1)]), (*z, [(1, 0, 1)]), (*x, [(0, 2, 0)])]
    return bounds, groups, sends


def shards(mesh, samples, owner):
    gx, gy = mesh.shape["gx"], mesh.shape["gy"]
    slots = owner.shape[0] // (gx * gy)
    rows = samples.shape[0]
    features = samples.shape[1] * gx * gy
    extra = -(-(rows // LANES) // 8) * 8
    per = slots * HALF + extra
    bounds, groups, sends = plan(gx, gy, per)
    pieces = [atoms for _, group in groups for atoms in group]

    def pairs(axis, bit):
        if axis == "gx":
            return [(i * gy + j, (i ^ bit) * gy + j) for i in range(gx) for j in range(gy)]
        return [(i * gy + j, i * gy + (j ^ bit)) for i in range(gx) for j in range(gy)]

    tiles, squares = gram_tiles(samples, owner.shape[0], extra)
    pick = functools.partial(
        pick_tiles, owner, tiles, squares, bounds=bounds, columns=gy, slots=slots
    )
    arrays = []
    for _, group in groups:
        arrays += pick(pieces=group)
    index = tile_index(owner, slots, gy, rows // TILE)
    terms = {}
    for n, atoms in enumerate(pieces):
        at = 0
        for atom in atoms:
            terms[atom] = [(n, at)]
            at += bounds[atom[2]][1] - bounds[atom[2]][0]

    def runs(atoms):
        joined = []
        for atom in atoms:
            size = bounds[atom[2]][1] - bounds[atom[2]][0]
            mine = terms.pop(atom)
            if joined and [(i, lo - joined[-1][1]) for i, lo in mine] == joined[-1][0]:
                joined[-1][1] += size
            else:
                joined.append([list(mine), size])
        return joined

    def gather(joined):
        used = sorted({i for parts, _ in joined for i, _ in parts})
        local = {i: k for k, i in enumerate(used)}
        return [arrays[i] for i in used], tuple(
            (tuple((local[i], lo) for i, lo in parts), size) for parts, size in joined
        )

    for axis, bit, atoms in sends:
        values, joined = gather(runs(atoms))
        if len(values) == 1 and len(joined) == 1 and values[0].shape[0] == joined[0][1]:
            sent = values[0]
        else:
            sent = add_terms(values, joined)
        arrays.append(lax.ppermute(sent, AXES, pairs(axis, bit)))
        at = 0
        for x, y, k in atoms:
            there = (x & ~bit, y, k) if axis == "gx" else (x, y & ~bit, k)
            terms[there].append((len(arrays) - 1, at))
            at += bounds[k][1] - bounds[k][0]
    values, joined = gather(runs([(0, 0, k) for k in range(len(bounds))]))
    assert not terms
    return finish(index, values, joined, slots, features)


def solution(mesh):
    step = jax.shard_map(
        functools.partial(shards, mesh),
        mesh=mesh,
        in_specs=(P("grp", AXES), P()),
        out_specs=P(("grp", "gx", "gy"), None),
        check_vma=False,
    )
    _, _, _ = plan(mesh.shape["gx"], mesh.shape["gy"], 1024)
    return step
```

```python
import functools

import jax
import jax.numpy as jnp
from jax import lax
from jax.experimental import pallas as pl
from jax.experimental.pallas import tpu as pltpu
from jax.sharding import PartitionSpec as P


TILE = 64
HALF = TILE // 2
LANES = 2 * TILE
PITCH = HALF + 8
EPS = 1e-06
AXES = ("gx", "gy")


def row_cuts(rows):
    cuts = list(range(0, rows, 256))
    if len(cuts) > 1 and rows - cuts[-1] < 256:
        cuts.pop()
    return tuple(zip(cuts, cuts[1:] + [rows]))


def gram_kernel(cuts, spans, hbm_ref, tiles, squares, x_ref, g_ref, sems):
    copies = [
        pltpu.make_async_copy(hbm_ref.at[:, pl.ds(lo, hi - lo)], x_ref.at[:, pl.ds(lo, hi - lo)], sems.at[n])
        for n, (lo, hi) in enumerate(spans)
    ]
    for copy in copies:
        copy.start()
    left = lax.broadcasted_iota(jnp.int32, (HALF, LANES), 1) < TILE
    eye = lax.broadcasted_iota(jnp.int32, (LANES, LANES), 0) == lax.broadcasted_iota(jnp.int32, (LANES, LANES), 1)
    diagonal = []
    for n, (k0, k1) in enumerate(spans):
        copies[n].wait()
        for m, (r0, r1) in enumerate(cuts):
            for c0, c1 in cuts[: m + 1]:
                block = lax.dot_general(
                    x_ref[r0:r1, k0:k1], x_ref[c0:c1, k0:k1], (((1,), (1,)), ((), ())), preferred_element_type=jnp.float32
                )
                if n:
                    block = g_ref[r0:r1, c0:c1] + block
                g_ref[r0:r1, c0:c1] = block
                if n + 1 < len(spans):
                    continue
                for row in range(r0 // TILE, r1 // TILE):
                    for b in range(c0 // LANES, c1 // LANES):
                        col = 2 * b
                        if col > row:
                            continue
                        lanes = slice(b * LANES, (b + 1) * LANES)
                        upper = g_ref[row * TILE : row * TILE + HALF, lanes]
                        lower = g_ref[row * TILE + HALF : (row + 1) * TILE, lanes]
                        at = (row * (row + 1) // 2 + col) * HALF
                        tiles[at : at + HALF, :] = jnp.where(left, upper, pltpu.roll(lower, TILE, 1))
                        if col + 1 <= row:
                            tiles[at + HALF : at + 2 * HALF, :] = jnp.where(left, pltpu.roll(upper, TILE, 1), lower)
            if n + 1 == len(spans):
                for b in range(r0 // LANES, r1 // LANES):
                    part = g_ref[b * LANES : (b + 1) * LANES, b * LANES : (b + 1) * LANES]
                    diagonal.append(jnp.sum(jnp.where(eye, part, 0.0), axis=0, keepdims=True))
    high = cuts[-1][1] // TILE
    live = high * (high + 1) // 2 * HALF
    tiles[live:, :] = jnp.zeros((tiles.shape[0] - live, LANES), jnp.float32)
    extra = squares.shape[0]
    squares[...] = jnp.concatenate(diagonal + [jnp.zeros((extra - len(diagonal), LANES), jnp.float32)], axis=0)


def gram_tiles(samples, count, extra):
    rows, features = samples.shape
    cuts = row_cuts(rows)
    first = features // 4
    spans = ((0, first), (first, features)) if first % LANES == 0 else ((0, features),)
    vmem = pl.BlockSpec(memory_space=pltpu.VMEM)
    return pl.pallas_call(
        functools.partial(gram_kernel, cuts, spans),
        out_shape=[
            jax.ShapeDtypeStruct((count * HALF, LANES), jnp.float32),
            jax.ShapeDtypeStruct((extra, LANES), jnp.float32),
        ],
        in_specs=[pl.BlockSpec(memory_space=pltpu.HBM)],
        out_specs=[vmem] * 2,
        scratch_shapes=[
            pltpu.VMEM((rows, features), samples.dtype),
            pltpu.VMEM((rows, rows), jnp.float32),
            pltpu.SemaphoreType.DMA((len(spans),)),
        ],
        compiler_params=pltpu.CompilerParams(vmem_limit_bytes=44 * 2**20),
        cost_estimate=pl.CostEstimate(
            flops=rows * rows * features, bytes_accessed=rows * features * 2 + count * HALF * LANES * 4, transcendentals=0
        ),
        name="gram_tiles",
    )(samples)


def pick_kernel(pieces, bounds, columns, slots, owner_ref, tiles, squares, *outs):
    at_x, at_y = lax.axis_index("gx"), lax.axis_index("gy")
    for out, atoms in zip(outs, pieces):
        at = 0
        for far_x, far_y, k in atoms:
            dest = (at_x ^ far_x) * columns + (at_y ^ far_y)
            lo, hi = bounds[k]
            for i in range(lo // HALF, min(hi // HALF, slots)):
                source = pl.multiple_of(owner_ref[dest * slots + i] * HALF, HALF)
                out[at : at + HALF, :] = tiles[pl.ds(source, HALF), :]
                at += HALF
            if hi == bounds[-1][1]:
                out[at : at + squares.shape[0], :] = squares[...]
                at += squares.shape[0]


def pick_tiles(owner, tiles, squares, pieces, bounds, columns, slots):
    sizes = [sum(bounds[k][1] - bounds[k][0] for _, _, k in atoms) for atoms in pieces]
    vmem, smem = pl.BlockSpec(memory_space=pltpu.VMEM), pl.BlockSpec(memory_space=pltpu.SMEM)
    return pl.pallas_call(
        functools.partial(pick_kernel, pieces, bounds, columns, slots),
        out_shape=[jax.ShapeDtypeStruct((size, LANES), jnp.float32) for size in sizes],
        in_specs=[smem, vmem, vmem],
        out_specs=[vmem] * len(sizes),
        compiler_params=pltpu.CompilerParams(vmem_limit_bytes=2**20),
        cost_estimate=pl.CostEstimate(flops=10**6, bytes_accessed=sum(sizes) * LANES * 8, transcendentals=0),
        name="pick_tiles",
    )(owner, tiles, squares)


def finish_kernel(joined, slots, features, index_ref, *refs):
    out_hbm, total, inv, rows_of, cols_of, packed, out_ref, sems = refs[-8:]
    add_kernel(joined, *refs[:-8], total)
    meansq = total[slots * HALF :, :] / features + EPS
    inv[...] = 1.0 / jnp.sqrt(meansq)
    half = lax.broadcasted_iota(jnp.int32, (1, LANES), 1) < TILE

    def pick(tile):
        line = inv[pl.ds(lax.div(tile, 2), 1), :]
        turned = pltpu.roll(line, TILE, 1)
        odd = lax.rem(tile, 2) == 1
        return jnp.where(odd, turned, line), jnp.where(odd, line, turned)

    rows_of[...] = jnp.zeros_like(rows_of)
    for i in range(slots):
        first, second = pick(index_ref[i])
        rows_of[i : i + 1, :] = first
        first, second = pick(index_ref[slots + i])
        alive = index_ref[2 * slots + i] == 1
        cols_of[i : i + 1, :] = jnp.where(half, first, second)
    down = rows_of[...].T
    left = lax.broadcasted_iota(jnp.int32, (HALF, LANES), 1) < TILE
    norm = 1.0 / features**0.5
    for i in range(slots):
        by_row = jnp.where(left, down[:HALF, i : i + 1], down[HALF:TILE, i : i + 1])
        scaled = total[i * HALF : (i + 1) * HALF, :] * by_row * (cols_of[i : i + 1, :] * norm)
        alive = index_ref[2 * slots + i] == 1
        packed[i * PITCH : i * PITCH + HALF, :] = jnp.where(alive, scaled, 0.0)
    step = min(slots, 8)
    wide = lax.broadcasted_iota(jnp.int32, (step, LANES), 1) < TILE
    copies = []
    for s in range(0, slots, step):
        for j in range(HALF):
            q = (2 * j) % HALF
            even = packed[pl.ds(s * PITCH + q, step, stride=PITCH), :]
            odd = packed[pl.ds(s * PITCH + q + 1, step, stride=PITCH), :]
            if 2 * j < HALF:
                line = jnp.where(wide, even, pltpu.roll(odd, TILE, 1))
            else:
                line = jnp.where(wide, pltpu.roll(even, TILE, 1), odd)
            out_ref[s : s + step, j * LANES : (j + 1) * LANES] = line
        copy = pltpu.make_async_copy(out_ref.at[pl.ds(s, step)], out_hbm.at[pl.ds(s, step)], sems.at[s // step])
        copy.start()
        copies.append(copy)
    for copy in copies:
        copy.wait()


def finish(index, arrays, joined, slots, features):
    per = sum(size for _, size in joined)
    extra = per - slots * HALF
    vmem = pl.BlockSpec(memory_space=pltpu.VMEM)
    return pl.pallas_call(
        functools.partial(finish_kernel, joined, slots, features),
        out_shape=jax.ShapeDtypeStruct((slots, TILE * TILE), jnp.float32),
        in_specs=[pl.BlockSpec(memory_space=pltpu.SMEM)] + [vmem] * len(arrays),
        out_specs=pl.BlockSpec(memory_space=pltpu.HBM),
        scratch_shapes=[
            pltpu.VMEM((per, LANES), jnp.float32),
            pltpu.VMEM((extra, LANES), jnp.float32),
            pltpu.VMEM((LANES, LANES), jnp.float32),
            pltpu.VMEM((max(slots, 8), LANES), jnp.float32),
            pltpu.VMEM((slots * PITCH, LANES), jnp.float32),
            pltpu.VMEM((slots, TILE * TILE), jnp.float32),
            pltpu.SemaphoreType.DMA((-(-slots // 8),)),
        ],
        compiler_params=pltpu.CompilerParams(vmem_limit_bytes=6 * 2**20),
        cost_estimate=pl.CostEstimate(flops=per * LANES * 8, bytes_accessed=per * LANES * 32, transcendentals=0),
        name="finish_tiles",
    )(index, *arrays)


def add_kernel(joined, *refs):
    at = 0
    for parts, size in joined:
        value = refs[parts[0][0]][parts[0][1] : parts[0][1] + size, :]
        for i, lo in parts[1:]:
            value = value + refs[i][lo : lo + size, :]
        refs[-1][at : at + size, :] = value
        at += size


def add_terms(arrays, joined):
    rows = sum(size for _, size in joined)
    vmem = pl.BlockSpec(memory_space=pltpu.VMEM)
    return pl.pallas_call(
        functools.partial(add_kernel, joined),
        out_shape=jax.ShapeDtypeStruct((rows, LANES), jnp.float32),
        in_specs=[vmem] * len(arrays),
        out_specs=vmem,
        compiler_params=pltpu.CompilerParams(vmem_limit_bytes=2 * 2**20),
        cost_estimate=pl.CostEstimate(flops=rows * LANES * 3, bytes_accessed=rows * LANES * 16, transcendentals=0),
        name="add_terms",
    )(*arrays)


def index_kernel(slots, columns, firsts, owner_ref, out_ref):
    at = (lax.axis_index("gx") * columns + lax.axis_index("gy")) * slots
    for i in range(slots):
        tile = owner_ref[at + i]
        row = jnp.int32(0)
        for first in firsts[1:-1]:
            row = row + (tile >= first).astype(jnp.int32)
        alive = tile < firsts[-1]
        out_ref[i] = jnp.where(alive, row, 0)
        out_ref[slots + i] = jnp.where(alive, tile - row * (row + 1) // 2, 0)
        out_ref[2 * slots + i] = alive.astype(jnp.int32)


def tile_index(owner, slots, columns, side):
    smem = pl.BlockSpec(memory_space=pltpu.SMEM)
    firsts = tuple(k * (k + 1) // 2 for k in range(side + 1))
    return pl.pallas_call(
        functools.partial(index_kernel, slots, columns, firsts),
        out_shape=jax.ShapeDtypeStruct((3 * slots,), jnp.int32),
        in_specs=[smem],
        out_specs=smem,
        compiler_params=pltpu.CompilerParams(vmem_limit_bytes=2**20),
        cost_estimate=pl.CostEstimate(flops=10**6, bytes_accessed=2**10, transcendentals=0),
        name="tile_index",
    )(owner)


def cut(per, parts):
    total = sum(parts)
    marks = [0]
    for part in parts:
        marks.append(marks[-1] + part)
    marks = [mark * per // total // HALF * HALF for mark in marks[:-1]] + [per]
    return list(zip(marks, marks[1:]))


def halving(gx, gy, per):
    bounds = cut(per, [1])
    blocks = [(x, y, 0) for y in range(gy) for x in range(gx)]
    pieces, sends = [], []
    for axis, size in (("gy", gy), ("gx", gx)):
        for bit in (1 << b for b in range(size.bit_length() - 1)):
            far = [block for block in blocks if (block[1] if axis == "gy" else block[0]) & bit]
            blocks = [block for block in blocks if block not in far]
            pieces = pieces or [(0, [far]), (1, [blocks])]
            sends.append((axis, bit, far))
    return bounds, pieces, sends


def plan(gx, gy, per):
    if (gx, gy) != (4, 4):
        return halving(gx, gy, per)
    core, x, z, zz = ("gy", 1), ("gy", 2), ("gx", 1), ("gx", 2)
    bounds = cut(per, [1, 3])
    sent = [
        [(3, 3, 1)],
        [(3, 3, 0), (1, 3, 0), (3, 1, 0), (1, 1, 0)],
        [(2, 3, 1)],
        [(1, 3, 1), (0, 3, 1)],
        [(2, 3, 0), (2, 1, 0), (0, 3, 0), (0, 1, 0)],
        [(r, 1, 1) for r in range(4)],
    ]
    kept = [[(r, y & 2, k) for r, y, k in atoms] for atoms in sent]
    groups = [(0, sent), (2, kept)]
    first, second, *others = [(*core, atoms) for atoms in sent]
    sends = [first, second, (*x, [(3, 2, 1)]), (*z, [(3, 2, 0), (1, 2, 0), (3, 0, 0), (1, 0, 0)]), *others]
    sends += [(*x, [(r, 2, 1)]) for r in (2, 1, 0)]
    sends += [(*z, [(3, 0, 1)]), (*zz, [(2, 2, 0), (2, 0, 0)]), (*zz, [(2, 0, 1)]), (*z, [(1, 0, 1)]), (*x, [(0, 2, 0)])]
    return bounds, groups, sends


def shards(mesh, samples, owner):
    gx, gy = mesh.shape["gx"], mesh.shape["gy"]
    slots = owner.shape[0] // (gx * gy)
    rows = samples.shape[0]
    features = samples.shape[1] * gx * gy
    extra = -(-(rows // LANES) // 8) * 8
    per = slots * HALF + extra
    bounds, groups, sends = plan(gx, gy, per)
    pieces = [atoms for _, group in groups for atoms in group]

    def pairs(axis, bit):
        if axis == "gx":
            return [(i * gy + j, (i ^ bit) * gy + j) for i in range(gx) for j in range(gy)]
        return [(i * gy + j, i * gy + (j ^ bit)) for i in range(gx) for j in range(gy)]

    tiles, squares = gram_tiles(samples, owner.shape[0], extra)
    pick = functools.partial(
        pick_tiles, owner, tiles, squares, bounds=bounds, columns=gy, slots=slots
    )
    arrays = []
    for _, group in groups:
        arrays += pick(pieces=group)
    index = tile_index(owner, slots, gy, rows // TILE)
    terms = {}
    for n, atoms in enumerate(pieces):
        at = 0
        for atom in atoms:
            terms[atom] = [(n, at)]
            at += bounds[atom[2]][1] - bounds[atom[2]][0]

    def runs(atoms):
        joined = []
        for atom in atoms:
            size = bounds[atom[2]][1] - bounds[atom[2]][0]
            mine = terms.pop(atom)
            if joined and [(i, lo - joined[-1][1]) for i, lo in mine] == joined[-1][0]:
                joined[-1][1] += size
            else:
                joined.append([list(mine), size])
        return joined

    def gather(joined):
        used = sorted({i for parts, _ in joined for i, _ in parts})
        local = {i: k for k, i in enumerate(used)}
        return [arrays[i] for i in used], tuple(
            (tuple((local[i], lo) for i, lo in parts), size) for parts, size in joined
        )

    for axis, bit, atoms in sends:
        values, joined = gather(runs(atoms))
        if len(values) == 1 and len(joined) == 1 and values[0].shape[0] == joined[0][1]:
            sent = values[0]
        else:
            sent = add_terms(values, joined)
        arrays.append(lax.ppermute(sent, AXES, pairs(axis, bit)))
        at = 0
        for x, y, k in atoms:
            there = (x & ~bit, y, k) if axis == "gx" else (x, y & ~bit, k)
            terms[there].append((len(arrays) - 1, at))
            at += bounds[k][1] - bounds[k][0]
    values, joined = gather(runs([(0, 0, k) for k in range(len(bounds))]))
    assert not terms
    return finish(index, values, joined, slots, features)


def solution(mesh):
    step = jax.shard_map(
        functools.partial(shards, mesh),
        mesh=mesh,
        in_specs=(P("grp", AXES), P()),
        out_specs=P(("grp", "gx", "gy"), None),
        check_vma=False,
    )
    _, _, _ = plan(mesh.shape["gx"], mesh.shape["gy"], 1024)
    return step
```
